128 devices in a mesh: coarse: 2 (over z_hi), fine: 8 (over z_lo, y), model: 8 (over x, core).
Axes of the slice: x: 4, y: 4, z: 4 (z_hi: 2, z_lo: 2; z = z_hi * 2 + z_lo), core: 2. Of those that a mesh axis runs over, the one named last changes fastest.
Arguments:
- fresh_keys: bfloat16 [16, 24576, 8, 128], P(None, ('coarse', 'fine'), 'model'), may hold values from -6 to 6
- fresh_values: bfloat16 [16, 24576, 8, 128], P(None, ('coarse', 'fine'), 'model'), may hold values from -6 to 6
- turn_angle: float32 [24576, 64], replicated, may hold values from -3.140625 to 3.140625
Outputs:
- cache_keys: bfloat16 [16, 24576, 8, 128], P(('coarse', 'fine'), None, 'model')
- cache_values: bfloat16 [16, 24576, 8, 128], P(('coarse', 'fine'), None, 'model')
- page_high: bfloat16 [16, 768, 8, 128], P(('coarse', 'fine'), None, 'model')
- page_low: bfloat16 [16, 768, 8, 128], P(('coarse', 'fine'), None, 'model')
The draws below stay inside these ranges and needn't reach their ends.
All inputs are finite; a program needn't handle non-finite values.
Results may differ from the reference program's by a relative error of at most 0.001.
Values may be sent and summed in bfloat16 or wider, within the bound.
No kernel may reach another device: no remote copies, remote signals or barrier semaphores. Data moves between devices by JAX's collectives and lax.ppermute only.
A program may use at most 128 MiB of HBM per device.

```python
import jax
import jax.numpy as jnp

BATCH = 16
LENGTH = 24576
KV_HEADS = 8
HEAD_SIZE = 128
HALF_HEAD = 64
PAGE = 32


def block_levels(rng, shape, shards, least, largest):
    def one(dim, blocks):
        heights = jax.random.uniform(jax.random.fold_in(jax.random.fold_in(rng, 6), dim), (blocks,), jnp.float32, least / len(shards), largest / len(shards))
        return jnp.repeat(jnp.exp(heights), shape[dim] // blocks).reshape((-1,) + (1,) * (len(shape) - dim - 1))

    factor_of = one(*shards[0])
    for cut in shards[1:]:
        factor_of = factor_of * one(*cut)
    return factor_of


def normal_values(key, dims, width, reach, split=(), kind=jnp.bfloat16):
    array = jax.random.normal(key, dims, jnp.float32) * width
    if len(split) > 0:
        array = block_levels(key, dims, split, -0.22, 0.18) * array
    return jnp.clip(array, min=-reach, max=reach).astype(kind)


def setup_inputs(seed: int = 0) -> dict:
    streams_of = jax.random.split(jax.random.key(seed), 4)
    fresh_keys = normal_values(streams_of[0], (BATCH, LENGTH, KV_HEADS, HEAD_SIZE), 1.0, 6.0, ((1, 16), (2, 8)))
    fresh_values = normal_values(streams_of[1], (BATCH, LENGTH, KV_HEADS, HEAD_SIZE), 1.0, 6.0, ((1, 16), (2, 8)))
    turn_angle = jnp.clip(jax.random.uniform(streams_of[2], (LENGTH, HALF_HEAD), jnp.float32, -3.140625, 3.140625), -3.140625, 3.140625)
    return {"fresh_keys": fresh_keys, "fresh_values": fresh_values, "turn_angle": turn_angle}


def turn_pairs(vectors, angle):
    half = vectors.shape[-1] // 2
    cosine, sine = jnp.cos(angle)[None, :, None, :], jnp.sin(angle)[None, :, None, :]
    first, second = vectors[..., :half], vectors[..., half:]
    return jnp.concatenate([first * cosine - second * sine, second * cosine + first * sine], axis=-1)


def prepare_keys(plain_keys, angle):
    wide_keys = plain_keys.astype(jnp.float32)
    return turn_pairs(wide_keys, angle)


def reference(fresh_keys, fresh_values, turn_angle):
    turned_keys = prepare_keys(fresh_keys, turn_angle)
    narrow_keys = turned_keys.astype(jnp.bfloat16)
    page_view = narrow_keys.reshape(BATCH, LENGTH // PAGE, PAGE, KV_HEADS, HEAD_SIZE)
    page_high = jnp.max(page_view, axis=2)
    page_low = jnp.min(page_view, axis=2)
    cache_keys = narrow_keys
    cache_values = fresh_values
    return cache_keys, cache_values, page_high, page_low
```

```python
import functools

import jax
import jax.numpy as jnp
from jax import lax
from jax.experimental import pallas as pl
from jax.experimental.pallas import tpu as pltpu
from jax.sharding import PartitionSpec as P

PAGE = 32
SEQ = ("coarse", "fine")
ROWS = 16
ANY = pl.BlockSpec(memory_space=pl.ANY)


def cos_sin(a):
    j = jnp.floor(a * 0.636619772367581 + 0.5)
    r = a - j * 1.5703125
    r = r - j * 4.837512969970703e-4
    r = r - j * 7.549789948768648e-8
    z = r * r
    s = r + r * z * (-1.6666654611e-1 + z * (8.3321608736e-3 + z * -1.9515295891e-4))
    c = 1.0 - 0.5 * z + z * z * (4.166664568298827e-2 + z * (-1.388731625493765e-3 + z * 2.443315711809948e-5))
    odd = jnp.abs(j) == 1.0
    near_c = jnp.where(odd, s, c)
    near_s = jnp.where(odd, c, s)
    cosine = jnp.where(j == 0.0, near_c, jnp.where(j == -1.0, near_c, -near_c))
    sine = jnp.where(j == 0.0, near_s, jnp.where(j == 1.0, near_s, -near_s))
    return cosine, sine


def head_kernel(shards, keys, values, angles, out, raw, turn, wide_c, wide_s, key_sem, value_sem, angle_sem):
    seqs, n, _ = keys.shape
    half = turn.shape[0]
    me = lax.axis_index("coarse") * shards + lax.axis_index("fine")
    angle_in = pltpu.make_async_copy(angles.at[:, pl.ds(pl.multiple_of(me * n, n), n)], turn, angle_sem)
    angle_in.start()
    key_in = [pltpu.make_async_copy(keys.at[b], raw.at[b], key_sem.at[b]) for b in range(seqs)]
    value_in = [pltpu.make_async_copy(values.at[b], out.at[b, 1], value_sem.at[b]) for b in range(seqs)]
    for copy in key_in + value_in:
        copy.start()
    angle_in.wait()

    def spread(t, _):
        at = pl.multiple_of(t * 128, 128)
        c, s = cos_sin(turn[:, pl.ds(at, 128)])
        wide_c[pl.ds(at, 128), :] = jnp.concatenate([c, c], axis=0).T
        wide_s[pl.ds(at, 128), :] = jnp.concatenate([-s, s], axis=0).T
        return 0

    lax.fori_loop(0, n // 128, spread, 0)
    group = 4
    for first in range(0, seqs, group):
        for b in range(first, first + group):
            key_in[b].wait()

        def rows(t, _):
            at = pl.ds(pl.multiple_of(t * ROWS, ROWS), ROWS)
            c, s = wide_c[at, :], wide_s[at, :]
            for b in range(first, first + group):
                x = raw[b, at, :].astype(jnp.float32)
                out[b, 0, at, :] = (x * c + pltpu.roll(x, half, 1) * s).astype(jnp.bfloat16)
            return 0

        lax.fori_loop(0, n // ROWS, rows, 0, unroll=2)
    for copy in value_in:
        copy.wait()


def head(keys, values, angles, shards):
    seqs, n, size = keys.shape
    f32 = jnp.float32
    return pl.pallas_call(
        functools.partial(head_kernel, shards),
        out_shape=pltpu.VMEM((seqs, 2, n, size), jnp.bfloat16),
        in_specs=[ANY] * 3,
        out_specs=pl.BlockSpec(memory_space=pltpu.VMEM),
        scratch_shapes=[
            pltpu.VMEM((seqs, n, size), jnp.bfloat16),
            pltpu.VMEM((size // 2, n), f32),
            pltpu.VMEM((n, size), f32),
            pltpu.VMEM((n, size), f32),
            pltpu.SemaphoreType.DMA((seqs,)),
            pltpu.SemaphoreType.DMA((seqs,)),
            pltpu.SemaphoreType.DMA,
        ],
        compiler_params=pltpu.CompilerParams(vmem_limit_bytes=30 << 20),
        name="head",
    )(*[pltpu.with_memory_space_constraint(a, pltpu.HBM) for a in (keys, values, angles)])


def tail_kernel(moved, keys, values, high, low, sem):
    d, _, n, _ = moved.shape
    copies = []
    for b in range(d):
        copies.append(pltpu.make_async_copy(moved.at[b, 0], keys.at[pl.ds(b * n, n)], sem.at[0, b]))
        copies.append(pltpu.make_async_copy(moved.at[b, 1], values.at[pl.ds(b * n, n)], sem.at[1, b]))
    for copy in copies:
        copy.start()
    pages = 16
    per = n // (pages * PAGE)

    def reduce(t, _):
        b, q = t // per, t % per
        rows = moved[b, 0, pl.ds(pl.multiple_of(q * pages * PAGE, pages * PAGE), pages * PAGE), :]
        rows = rows.reshape(pages, PAGE, rows.shape[-1])
        at = pl.ds(pl.multiple_of(t * pages, pages), pages)
        high[at, :] = jnp.max(rows, axis=1)
        low[at, :] = jnp.min(rows, axis=1)
        return 0

    lax.fori_loop(0, d * per, reduce, 0)
    for copy in copies:
        copy.wait()


def tail(moved):
    d, _, n, size = moved.shape
    bf16 = jnp.bfloat16
    return pl.pallas_call(
        tail_kernel,
        out_shape=[
            jax.ShapeDtypeStruct((d * n, size), bf16),
            jax.ShapeDtypeStruct((d * n, size), bf16),
            jax.ShapeDtypeStruct((d * n // PAGE, size), bf16),
            jax.ShapeDtypeStruct((d * n // PAGE, size), bf16),
        ],
        in_specs=[pl.BlockSpec(memory_space=pltpu.VMEM)],
        out_specs=[ANY, ANY, pl.BlockSpec(memory_space=pltpu.VMEM), pl.BlockSpec(memory_space=pltpu.VMEM)],
        scratch_shapes=[pltpu.SemaphoreType.DMA((2, d))],
        compiler_params=pltpu.CompilerParams(vmem_limit_bytes=16 << 20),
        name="tail",
    )(pltpu.with_memory_space_constraint(moved, pltpu.VMEM))


def solution(mesh):
    shards = mesh.shape["fine"]

    def on_device(fresh_keys, fresh_values, turn_angle):
        sent = head(fresh_keys[:, :, 0], fresh_values[:, :, 0], turn_angle.T, shards)
        moved = lax.all_to_all(sent, SEQ, split_axis=0, concat_axis=0, tiled=True)
        keys, values, high, low = tail(moved)
        return tuple(a[None, :, None] for a in (keys, values, high, low))

    cut = P(None, SEQ, "model", None)
    out = P(SEQ, None, "model", None)
    return jax.shard_map(
        on_device, mesh=mesh, in_specs=(cut, cut, P()), out_specs=(out,) * 4, check_vma=False
    )
```

```python
import functools
from typing import Any, NamedTuple

import jax
import jax.numpy as jnp
from jax import lax
from jax.experimental import pallas as pl
from jax.experimental.pallas import tpu as pltpu
from jax.sharding import PartitionSpec as P

PAGE = 32
SEQ = ("coarse", "fine")
SIDE = 4
COST = 50_000_000
ROWS = 32
UNROLL = 2
BF16 = jnp.bfloat16
VMEM_LIMIT = 20 << 20


def place():
    me = lax.axis_index("coarse") * lax.axis_size("fine") + lax.axis_index("fine")
    return me % SIDE, me // SIDE


def slot(y, z):
    return (z + 2 * SIDE) % SIDE * SIDE + (y + 2 * SIDE) % SIDE


def shift(a, dy, dz):
    pairs = [(i, slot(i % SIDE + dy, i // SIDE + dz)) for i in range(SIDE * SIDE)]
    return lax.ppermute(a, SEQ, pairs)


def cos_sin(a):
    j = jnp.floor(a * 0.636619772367581 + 0.5)
    r = a - j * 1.5703125
    r = r - j * 4.837512969970703e-4
    r = r - j * 7.549789948768648e-8
    z = r * r
    s = r + r * z * (-1.6666654611e-1 + z * (8.3321608736e-3 + z * -1.9515295891e-4))
    c = 1.0 - 0.5 * z + z * z * (4.166664568298827e-2 + z * (-1.388731625493765e-3 + z * 2.443315711809948e-5))
    odd = jnp.abs(j) == 1.0
    near_c = jnp.where(odd, s, c)
    near_s = jnp.where(odd, c, s)
    cosine = jnp.where(j == 0.0, near_c, jnp.where(j == -1.0, near_c, -near_c))
    sine = jnp.where(j == 0.0, near_s, jnp.where(j == 1.0, near_s, -near_s))
    return cosine, sine


class Task(NamedTuple):
    read: int
    block: Any
    to: int
    index: Any
    turn: Any = None
    rows: bool = False
    pages: bool = False


def value_at(index, y, z):
    return index(y, z) if callable(index) else index


def step_kernel(far, near, writes, skip, tasks, turns, *refs):
    inputs, refs = refs[: far + near], refs[far + near :]
    if turns:
        angles, refs = refs[0], refs[1:]
    outs, refs = refs[skip : skip + writes], refs[skip + writes :]
    held, turned, high, low, raw_angle, wide_c, wide_s, in_sem, out_sem, page_sem, angle_sem = refs
    n, size = held.shape[1:]
    y, z = place()
    angle_loads, loads, ready, stores = [], {}, {}, []
    h = 0
    for t, e in enumerate(turns):
        first = pl.multiple_of(slot(y - e, z) * n, n)
        angle_loads.append(pltpu.make_async_copy(angles.at[:, pl.ds(first, n)], raw_angle.at[t], angle_sem.at[t]))
    for k, task in enumerate(tasks):
        source = inputs[task.read].at[value_at(task.block, y, z)]
        if task.read >= far:
            ready[k] = source
            continue
        direct = task.turn is None and not task.rows
        if direct:
            ready[k] = outs[task.to].at[task.index]
        else:
            ready[k] = held.at[h]
            h += 1
        loads[k] = pltpu.make_async_copy(source, ready[k], in_sem.at[len(loads)])
    for load in angle_loads + list(loads.values()):
        load.start()
    for t in range(len(turns)):
        angle_loads[t].wait()

        def spread(q, _, t=t):
            lanes = pl.ds(pl.multiple_of(q * 128, 128), 128)
            c, s = cos_sin(raw_angle[t, :, lanes])
            wide_c[t, lanes, :] = jnp.concatenate([c, c], axis=0).T
            wide_s[t, lanes, :] = jnp.concatenate([-s, s], axis=0).T
            return 0

        lax.fori_loop(0, n // 128, spread, 0)
    m = p = 0
    target = {}
    for t, e in enumerate(turns):
        group = [k for k, task in enumerate(tasks) if task.turn == e]
        for k in group:
            if tasks[k].rows:
                target[k] = turned.at[m]
                m += 1
            else:
                target[k] = outs[tasks[k].to].at[tasks[k].index]
            if k in loads:
                loads.pop(k).wait()

        def rotate(q, _, t=t, group=group):
            r = pl.ds(pl.multiple_of(q * ROWS, ROWS), ROWS)
            c, s = wide_c[t, r, :], wide_s[t, r, :]
            x = [ready[k][r, :].astype(jnp.float32) for k in group]
            w = [pltpu.roll(v, size // 2, 1) for v in x]
            for k, v, u in zip(group, x, w):
                target[k][r, :] = (v * c + u * s).astype(BF16)
            return 0

        lax.fori_loop(0, n // ROWS, rotate, 0, unroll=UNROLL)
    for k, task in enumerate(tasks):
        if k in loads:
            loads[k].wait()
        block = ready[k]
        if task.turn is not None:
            block = target[k]
        elif not task.rows and k not in loads:
            to = outs[task.to].at[task.index]

            def copy(q, _, block=block, to=to):
                r = pl.ds(pl.multiple_of(q * 256, 256), 256)
                to[r, :] = block[r, :]
                return 0

            lax.fori_loop(0, n // 256, copy, 0)
        if not task.rows:
            continue
        index = value_at(task.index, y, z)
        to = outs[task.to].at[pl.ds(pl.multiple_of(index * n, n), n)]
        stores.append(pltpu.make_async_copy(block, to, out_sem.at[k]))
        stores[-1].start()
        if task.pages:
            count, group = n // PAGE, 16

            def bound(q, _, block=block, p=p):
                rows = block[pl.ds(pl.multiple_of(q * group * PAGE, group * PAGE), group * PAGE), :]
                rows = rows.reshape(group, PAGE, size)
                r = pl.ds(pl.multiple_of(q * group, group), group)
                high[p, r, :] = jnp.max(rows, axis=1)
                low[p, r, :] = jnp.min(rows, axis=1)
                return 0

            lax.fori_loop(0, count // group, bound, 0)
            for i, side in enumerate((high, low)):
                to = outs[writes - 2 + i].at[pl.ds(pl.multiple_of(index * count, 16), count)]
                stores.append(pltpu.make_async_copy(side.at[p], to, page_sem.at[i, p]))
                stores[-1].start()
            p += 1
    for store in stores:
        store.wait()


def step(far, near, angles, sent, grown, tasks):
    n, size = (*far, *near)[0].shape[-2:]
    turns = sorted({t.turn for t in tasks if t.turn is not None})
    hbm, vmem = pl.BlockSpec(memory_space=pl.ANY), pl.BlockSpec(memory_space=pltpu.VMEM)
    operands = [pltpu.with_memory_space_constraint(a, pltpu.HBM) for a in far]
    operands += [pltpu.with_memory_space_constraint(a, pltpu.VMEM) for a in near]
    in_specs = [hbm] * len(far) + [vmem] * len(near)
    if turns:
        operands.append(pltpu.with_memory_space_constraint(angles, pltpu.HBM))
        in_specs.append(hbm)
    out = [pltpu.VMEM((c, n, size), BF16) for c in sent]
    out_specs = [vmem] * len(sent) + [hbm] * len(grown)
    aliases = {}
    for a in grown:
        if hasattr(a, "dtype"):
            aliases[len(operands)] = len(out)
            operands.append(a)
            in_specs.append(hbm)
            a = a.shape
        out.append(jax.ShapeDtypeStruct(a, BF16))
    t = max(len(turns), 1)
    held = max(sum(k.read < len(far) and (k.turn is not None or k.rows) for k in tasks), 1)
    loads = max(sum(k.read < len(far) for k in tasks), 1)
    m = max(sum(k.turn is not None and k.rows for k in tasks), 1)
    p = max(sum(k.pages for k in tasks), 1)
    f32 = jnp.float32
    return pl.pallas_call(
        functools.partial(step_kernel, len(far), len(near), len(out), len(aliases), tasks, turns),
        out_shape=out,
        in_specs=in_specs,
        out_specs=out_specs,
        input_output_aliases=aliases,
        scratch_shapes=[
            pltpu.VMEM((held, n, size), BF16),
            pltpu.VMEM((m, n, size), BF16),
            pltpu.VMEM((p, n // PAGE, size), BF16),
            pltpu.VMEM((p, n // PAGE, size), BF16),
            pltpu.VMEM((t, size // 2, n), f32),
            pltpu.VMEM((t, n, size), f32),
            pltpu.VMEM((t, n, size), f32),
            pltpu.SemaphoreType.DMA((loads,)),
            pltpu.SemaphoreType.DMA((len(tasks),)),
            pltpu.SemaphoreType.DMA((2, p)),
            pltpu.SemaphoreType.DMA((t,)),
        ],
        cost_estimate=pl.CostEstimate(
            flops=COST * len(tasks), bytes_accessed=4 * len(tasks) * n * size, transcendentals=0
        ),
        compiler_params=pltpu.CompilerParams(vmem_limit_bytes=VMEM_LIMIT),
    )(*operands)


def on_device(fresh_keys, fresh_values, turn_angle):
    keys, values, angles = fresh_keys[:, :, 0], fresh_values[:, :, 0], turn_angle.T
    seqs, n, size = keys.shape
    grown = [(seqs * n, size)] * 2 + [(seqs * n // PAGE, size)] * 2
    near = (1, 3)

    def key_block(e, j):
        return lambda y, z: slot(y + e, z + j)

    def value_block(e, j):
        return lambda y, z: slot(y + j, z + e)

    def from_y(e, j):
        return lambda y, z: slot(y - e, z - j)

    def hop(sent, first, js):
        half = len(sent) // 2
        moved = [shift(a, e if first else 0, 0 if first else e) for a, e in zip(sent[:half], js)]
        return moved, [shift(a, 0 if first else e, e if first else 0) for a, e in zip(sent[half:], js)]

    def pick(es, js):
        tasks = []
        for i, e in enumerate(es):
            tasks += [Task(0, key_block(e, j), i, q) for q, j in enumerate(js)]
        for i, e in enumerate(es):
            tasks += [Task(1, value_block(e, j), len(es) + i, q) for q, j in enumerate(js)]
        sent = step((keys, values), (), None, [len(js)] * (2 * len(es)), [], tasks)
        return hop(sent, True, es)

    k_first, v_first = pick(near, (0,))
    k_rest, v_rest = pick(near, (1, 3, 2))
    second = (1, 3, 2)

    tasks = [Task(0, key_block(0, j), q, 0, 0) for q, j in enumerate(second)]
    tasks += [Task(1, value_block(0, j), 3 + q, 0) for q, j in enumerate(second)]
    tasks.append(Task(0, key_block(0, 0), 6, from_y(0, 0), 0, True, True))
    tasks.append(Task(1, value_block(0, 0), 7, from_y(0, 0), rows=True))
    *sent, a, b, c, d = step((keys, values), (), angles, [1] * 6, grown, tasks)
    grown = [a, b, c, d]
    k_own, v_own = hop(sent[:2] + sent[3:5], False, near)
    k_own2, v_own2 = hop(sent[2:3] + sent[5:6], False, (2,))
    k_far, v_far = pick((2,), (0, 1, 3, 2))

    near_in = (*k_first, *v_first, *k_rest, *v_rest)
    tasks = []
    for q in range(3):
        tasks += [Task(4 + i, q, q, i, e) for i, e in enumerate(near)]
        tasks += [Task(6 + i, q, 3 + q, i) for i, e in enumerate(near)]
    tasks += [Task(i, 0, 6, from_y(e, 0), e, True, True) for i, e in enumerate(near)]
    tasks += [Task(2 + i, 0, 7, from_y(0, e), rows=True) for i, e in enumerate(near)]
    *sent, a, b, c, d = step((), near_in, angles, [2] * 6, grown, tasks)
    grown = [a, b, c, d]
    k_near, v_near = hop(sent[:2] + sent[3:5], False, near)
    k_near2, v_near2 = hop(sent[2:3] + sent[5:6], False, (2,))

    tasks = [Task(0, 1 + q, q, 0, 2) for q in range(3)]
    tasks += [Task(1, 1 + q, 3 + q, 0) for q in range(3)]
    tasks.append(Task(0, 0, 6, from_y(2, 0), 2, True, True))
    tasks.append(Task(1, 0, 7, from_y(0, 2), rows=True))
    *sent, a, b, c, d = step((), (*k_far, *v_far), angles, [1] * 6, grown, tasks)
    grown = [a, b, c, d]
    k_last, v_last = hop(sent[:2] + sent[3:5], False, near)
    k_last2, v_last2 = hop(sent[2:3] + sent[5:6], False, (2,))

    def finish(got, grown):
        tasks, reads = [], []
        for k_got, v_got, js, es in got:
            for a, b, j in zip(k_got, v_got, js):
                at = len(reads)
                reads += [a, b]
                tasks += [Task(at, q, 0, from_y(e, j), None, True, True) for q, e in enumerate(es)]
                tasks += [Task(at + 1, q, 1, from_y(j, e), None, True) for q, e in enumerate(es)]
        return step((), reads, None, [], grown, tasks)

    grown = finish([(k_own, v_own, near, (0,)), (k_own2, v_own2, (2,), (0,))], grown)
    grown = finish([(k_near, v_near, near, near), (k_near2, v_near2, (2,), near)], grown)
    grown = finish([(k_last, v_last, near, (2,))], grown)
    grown = finish([(k_last2, v_last2, (2,), (2,))], grown)
    return tuple(x[None, :, None] for x in grown)


def solution(mesh):
    cut = P(None, SEQ, "model", None)
    out = P(SEQ, None, "model", None)

    return jax.shard_map(on_device, mesh=mesh, in_specs=(cut, cut, P()), out_specs=(out,) * 4, check_vma=False)
```

```python
import functools
from typing import Any, NamedTuple

import jax
import jax.numpy as jnp
from jax import lax
from jax.experimental import pallas as pl
from jax.experimental.pallas import tpu as pltpu
from jax.sharding import PartitionSpec as P

PAGE = 32
SEQ = ("coarse", "fine")
SIDE = 4
COST = 50_000_000
ROWS = 32
UNROLL = 2
BF16 = jnp.bfloat16
VMEM_LIMIT = 20 << 20


def place():
    me = lax.axis_index("coarse") * lax.axis_size("fine") + lax.axis_index("fine")
    return me % SIDE, me // SIDE


def slot(y, z):
    return (z + 2 * SIDE) % SIDE * SIDE + (y + 2 * SIDE) % SIDE


def shift(a, dy, dz):
    pairs = [(i, slot(i % SIDE + dy, i // SIDE + dz)) for i in range(SIDE * SIDE)]
    return lax.ppermute(a, SEQ, pairs)


def cos_sin(a):
    j = jnp.floor(a * 0.636619772367581 + 0.5)
    r = a - j * 1.5703125
    r = r - j * 4.837512969970703e-4
    r = r - j * 7.549789948768648e-8
    z = r * r
    s = r + r * z * (-1.6666654611e-1 + z * (8.3321608736e-3 + z * -1.9515295891e-4))
    c = 1.0 - 0.5 * z + z * z * (4.166664568298827e-2 + z * (-1.388731625493765e-3 + z * 2.443315711809948e-5))
    odd = jnp.abs(j) == 1.0
    near_c = jnp.where(odd, s, c)
    near_s = jnp.where(odd, c, s)
    cosine = jnp.where(j == 0.0, near_c, jnp.where(j == -1.0, near_c, -near_c))
    sine = jnp.where(j == 0.0, near_s, jnp.where(j == 1.0, near_s, -near_s))
    return cosine, sine


class Task(NamedTuple):
    read: int
    block: Any
    to: int
    index: Any
    turn: Any = None
    rows: bool = False
    pages: bool = False


def value_at(index, y, z):
    return index(y, z) if callable(index) else index


def step_kernel(far, near, writes, skip, tasks, turns, *refs):
    inputs, refs = refs[: far + near], refs[far + near :]
    if turns:
        angles, refs = refs[0], refs[1:]
    outs, refs = refs[skip : skip + writes], refs[skip + writes :]
    held, turned, high, low, raw_angle, wide_c, wide_s, in_sem, out_sem, page_sem, angle_sem = refs
    n, size = held.shape[1:]
    y, z = place()
    angle_loads, loads, ready, stores = [], {}, {}, []
    h = 0
    for t, e in enumerate(turns):
        first = pl.multiple_of(slot(y - e, z) * n, n)
        angle_loads.append(pltpu.make_async_copy(angles.at[:, pl.ds(first, n)], raw_angle.at[t], angle_sem.at[t]))
    for k, task in enumerate(tasks):
        source = inputs[task.read].at[value_at(task.block, y, z)]
        if task.read >= far:
            ready[k] = source
            continue
        direct = task.turn is None and not task.rows
        if direct:
            ready[k] = outs[task.to].at[task.index]
        else:
            ready[k] = held.at[h]
            h += 1
        loads[k] = pltpu.make_async_copy(source, ready[k], in_sem.at[len(loads)])
    for load in angle_loads + list(loads.values()):
        load.start()
    for t in range(len(turns)):
        angle_loads[t].wait()

        def spread(q, _, t=t):
            lanes = pl.ds(pl.multiple_of(q * 128, 128), 128)
            c, s = cos_sin(raw_angle[t, :, lanes])
            wide_c[t, lanes, :] = jnp.concatenate([c, c], axis=0).T
            wide_s[t, lanes, :] = jnp.concatenate([-s, s], axis=0).T
            return 0

        lax.fori_loop(0, n // 128, spread, 0)
    m = p = 0
    target = {}
    for t, e in enumerate(turns):
        group = [k for k, task in enumerate(tasks) if task.turn == e]
        for k in group:
            if tasks[k].rows:
                target[k] = turned.at[m]
                m += 1
            else:
                target[k] = outs[tasks[k].to].at[tasks[k].index]
            if k in loads:
                loads.pop(k).wait()

        def rotate(q, _, t=t, group=group):
            r = pl.ds(pl.multiple_of(q * ROWS, ROWS), ROWS)
            c, s = wide_c[t, r, :], wide_s[t, r, :]
            x = [ready[k][r, :].astype(jnp.float32) for k in group]
            w = [pltpu.roll(v, size // 2, 1) for v in x]
            for k, v, u in zip(group, x, w):
                target[k][r, :] = (v * c + u * s).astype(BF16)
            return 0

        lax.fori_loop(0, n // ROWS, rotate, 0, unroll=UNROLL)
    for k, task in enumerate(tasks):
        if k in loads:
            loads[k].wait()
        block = ready[k]
        if task.turn is not None:
            block = target[k]
        elif not task.rows and k not in loads:
            to = outs[task.to].at[task.index]

            def copy(q, _, block=block, to=to):
                r = pl.ds(pl.multiple_of(q * 256, 256), 256)
                to[r, :] = block[r, :]
                return 0

            lax.fori_loop(0, n // 256, copy, 0)
        if not task.rows:
            continue
        ready[k] = block
        index = value_at(task.index, y, z)
        to = outs[task.to].at[pl.ds(pl.multiple_of(index * n, n), n)]
        stores.append(pltpu.make_async_copy(block, to, out_sem.at[k]))
        stores[-1].start()
    count, group = n // PAGE, 16
    for k, task in enumerate(tasks):
        if not task.pages:
            continue

        def bound(q, _, block=ready[k], p=p):
            rows = block[pl.ds(pl.multiple_of(q * group * PAGE, group * PAGE), group * PAGE), :]
            rows = rows.reshape(group, PAGE, size)
            r = pl.ds(pl.multiple_of(q * group, group), group)
            high[p, r, :] = jnp.max(rows, axis=1)
            low[p, r, :] = jnp.min(rows, axis=1)
            return 0

        lax.fori_loop(0, count // group, bound, 0, unroll=True)
        for i, side in enumerate((high, low)):
            to = outs[writes - 2 + i].at[pl.ds(pl.multiple_of(value_at(task.index, y, z) * count, 16), count)]
            stores.append(pltpu.make_async_copy(side.at[p], to, page_sem.at[i, p]))
            stores[-1].start()
        p += 1
    for store in stores:
        store.wait()


def step(far, near, angles, sent, grown, tasks):
    n, size = (*far, *near)[0].shape[-2:]
    turns = sorted({t.turn for t in tasks if t.turn is not None})
    hbm, vmem = pl.BlockSpec(memory_space=pl.ANY), pl.BlockSpec(memory_space=pltpu.VMEM)
    operands = [pltpu.with_memory_space_constraint(a, pltpu.HBM) for a in far]
    operands += [pltpu.with_memory_space_constraint(a, pltpu.VMEM) for a in near]
    in_specs = [hbm] * len(far) + [vmem] * len(near)
    if turns:
        operands.append(pltpu.with_memory_space_constraint(angles, pltpu.HBM))
        in_specs.append(hbm)
    out = [pltpu.VMEM((c, n, size), BF16) for c in sent]
    out_specs = [vmem] * len(sent) + [hbm] * len(grown)
    aliases = {}
    for a in grown:
        if hasattr(a, "dtype"):
            aliases[len(operands)] = len(out)
            operands.append(a)
            in_specs.append(hbm)
            a = a.shape
        out.append(jax.ShapeDtypeStruct(a, BF16))
    t = max(len(turns), 1)
    held = max(sum(k.read < len(far) and (k.turn is not None or k.rows) for k in tasks), 1)
    loads = max(sum(k.read < len(far) for k in tasks), 1)
    m = max(sum(k.turn is not None and k.rows for k in tasks), 1)
    p = max(sum(k.pages for k in tasks), 1)
    f32 = jnp.float32
    return pl.pallas_call(
        functools.partial(step_kernel, len(far), len(near), len(out), len(aliases), tasks, turns),
        out_shape=out,
        in_specs=in_specs,
        out_specs=out_specs,
        input_output_aliases=aliases,
        scratch_shapes=[
            pltpu.VMEM((held, n, size), BF16),
            pltpu.VMEM((m, n, size), BF16),
            pltpu.VMEM((p, n // PAGE, size), BF16),
            pltpu.VMEM((p, n // PAGE, size), BF16),
            pltpu.VMEM((t, size // 2, n), f32),
            pltpu.VMEM((t, n, size), f32),
            pltpu.VMEM((t, n, size), f32),
            pltpu.SemaphoreType.DMA((loads,)),
            pltpu.SemaphoreType.DMA((len(tasks),)),
            pltpu.SemaphoreType.DMA((2, p)),
            pltpu.SemaphoreType.DMA((t,)),
        ],
        cost_estimate=pl.CostEstimate(
            flops=COST * len(tasks), bytes_accessed=4 * len(tasks) * n * size, transcendentals=0
        ),
        compiler_params=pltpu.CompilerParams(vmem_limit_bytes=VMEM_LIMIT),
    )(*operands)


def on_device(fresh_keys, fresh_values, turn_angle):
    keys, values, angles = fresh_keys[:, :, 0], fresh_values[:, :, 0], turn_angle.T
    seqs, n, size = keys.shape
    grown = [(seqs * n, size)] * 2 + [(seqs * n // PAGE, size)] * 2
    near = (1, 3)

    def key_block(e, j):
        return lambda y, z: slot(y + e, z + j)

    def value_block(e, j):
        return lambda y, z: slot(y + j, z + e)

    def from_y(e, j):
        return lambda y, z: slot(y - e, z - j)

    def hop(sent, first, js):
        half = len(sent) // 2
        moved = [shift(a, e if first else 0, 0 if first else e) for a, e in zip(sent[:half], js)]
        return moved, [shift(a, 0 if first else e, e if first else 0) for a, e in zip(sent[half:], js)]

    def pick(es, js):
        tasks = []
        for i, e in enumerate(es):
            tasks += [Task(0, key_block(e, j), i, q) for q, j in enumerate(js)]
        for i, e in enumerate(es):
            tasks += [Task(1, value_block(e, j), len(es) + i, q) for q, j in enumerate(js)]
        sent = step((keys, values), (), None, [len(js)] * (2 * len(es)), [], tasks)
        return hop(sent, True, es)

    k_first, v_first = pick((2,), (0, 1))
    k_rest, v_rest = pick(near, (0, 1, 3, 2))
    second = (1, 3, 2)

    tasks = [Task(0, key_block(0, j), q, 0, 0) for q, j in enumerate(second)]
    tasks += [Task(1, value_block(0, j), 3 + q, 0) for q, j in enumerate(second)]
    tasks.append(Task(0, key_block(0, 0), 6, from_y(0, 0), 0, True, True))
    tasks.append(Task(1, value_block(0, 0), 7, from_y(0, 0), rows=True))
    *sent, a, b, c, d = step((keys, values), (), angles, [1] * 6, grown, tasks)
    grown = [a, b, c, d]
    k_own, v_own = hop(sent[:2] + sent[3:5], False, near)
    k_own2, v_own2 = hop(sent[2:3] + sent[5:6], False, (2,))
    k_far, v_far = pick((2,), (3, 2))

    near_in = (*k_rest, *v_rest)
    tasks = []
    for q in range(3):
        tasks += [Task(i, 1 + q, q, i, e) for i, e in enumerate(near)]
        tasks += [Task(2 + i, 1 + q, 3 + q, i) for i, e in enumerate(near)]
    tasks += [Task(i, 0, 6, from_y(e, 0), e, True, True) for i, e in enumerate(near)]
    tasks += [Task(2 + i, 0, 7, from_y(0, e), rows=True) for i, e in enumerate(near)]
    *sent, a, b, c, d = step((), near_in, angles, [2] * 6, grown, tasks)
    grown = [a, b, c, d]
    k_near, v_near = hop(sent[:2] + sent[3:5], False, near)
    k_near2, v_near2 = hop(sent[2:3] + sent[5:6], False, (2,))

    parts = ((0, 1), (2, 0), (2, 1))
    tasks = [Task(i, at, q, 0, 2) for q, (i, at) in enumerate(parts)]
    tasks += [Task(i + 1, at, 3 + q, 0) for q, (i, at) in enumerate(parts)]
    tasks.append(Task(0, 0, 6, from_y(2, 0), 2, True, True))
    tasks.append(Task(1, 0, 7, from_y(0, 2), rows=True))
    far_in = (*k_first, *v_first, *k_far, *v_far)
    *sent, a, b, c, d = step((), far_in, angles, [1] * 6, grown, tasks)
    grown = [a, b, c, d]
    k_last, v_last = hop(sent[:2] + sent[3:5], False, near)
    k_last2, v_last2 = hop(sent[2:3] + sent[5:6], False, (2,))

    def finish(got, grown):
        tasks, reads = [], []
        for k_got, v_got, js, es in got:
            for a, b, j in zip(k_got, v_got, js):
                at = len(reads)
                reads += [a, b]
                tasks += [Task(at, q, 0, from_y(e, j), None, True, True) for q, e in enumerate(es)]
                tasks += [Task(at + 1, q, 1, from_y(j, e), None, True) for q, e in enumerate(es)]
        return step((), reads, None, [], grown, tasks)

    grown = finish([(k_own, v_own, near, (0,)), (k_own2, v_own2, (2,), (0,))], grown)
    grown = finish([(k_near, v_near, near, near), (k_near2, v_near2, (2,), near)], grown)
    grown = finish([(k_last, v_last, near, (2,))], grown)
    grown = finish([(k_last2, v_last2, (2,), (2,))], grown)
    return tuple(x[None, :, None] for x in grown)


def solution(mesh):
    cut = P(None, SEQ, "model", None)
    out = P(SEQ, None, "model", None)

    return jax.shard_map(on_device, mesh=mesh, in_specs=(cut, cut, P()), out_specs=(out,) * 4, check_vma=False)
```

```python
import functools
from typing import Any, NamedTuple

import jax
import jax.numpy as jnp
from jax import lax
from jax.experimental import pallas as pl
from jax.experimental.pallas import tpu as pltpu
from jax.sharding import PartitionSpec as P

PAGE = 32
SEQ = ("coarse", "fine")
SIDE = 4
COST = 50_000_000
ROWS = 32
UNROLL = 2
BF16 = jnp.bfloat16
VMEM_LIMIT = 20 << 20


def place():
    me = lax.axis_index("coarse") * lax.axis_size("fine") + lax.axis_index("fine")
    return me % SIDE, me // SIDE


def slot(y, z):
    return (z + 2 * SIDE) % SIDE * SIDE + (y + 2 * SIDE) % SIDE


def shift(a, dy, dz):
    pairs = [(i, slot(i % SIDE + dy, i // SIDE + dz)) for i in range(SIDE * SIDE)]
    return lax.ppermute(a, SEQ, pairs)


class Task(NamedTuple):
    read: int
    block: Any
    to: int
    index: Any
    turn: Any = None
    rows: bool = False
    pages: bool = False


def value_at(index, y, z):
    return index(y, z) if callable(index) else index


def step_kernel(far, near, writes, skip, tasks, turns, *refs):
    inputs, refs = refs[: far + near], refs[far + near :]
    if turns:
        angles, refs = refs[0], refs[1:]
    outs, refs = refs[skip : skip + writes], refs[skip + writes :]
    held, turned, high, low, raw_angle, wide_c, wide_s, in_sem, out_sem, page_sem, angle_sem = refs
    n, size = held.shape[1:]
    y, z = place()
    angle_loads, loads, ready, stores = [], {}, {}, []
    h = 0
    for t, e in enumerate(turns):
        first = pl.multiple_of(slot(y - e, z) * n, n)
        angle_loads.append(pltpu.make_async_copy(angles.at[:, pl.ds(first, n)], raw_angle.at[t], angle_sem.at[t]))
    for k, task in enumerate(tasks):
        source = inputs[task.read].at[value_at(task.block, y, z)]
        if task.read >= far:
            ready[k] = source
            continue
        direct = task.turn is None and not task.rows
        if direct:
            ready[k] = outs[task.to].at[task.index]
        else:
            ready[k] = held.at[h]
            h += 1
        loads[k] = pltpu.make_async_copy(source, ready[k], in_sem.at[len(loads)])
    for load in angle_loads + list(loads.values()):
        load.start()
    for t in range(len(turns)):
        angle_loads[t].wait()

        def spread(q, _, t=t):
            lanes = pl.ds(pl.multiple_of(q * 128, 128), 128)
            a = raw_angle[t, :, lanes]
            c, s = jnp.cos(a), jnp.sin(a)
            wide_c[t, lanes, :] = jnp.concatenate([c, c], axis=0).T
            wide_s[t, lanes, :] = jnp.concatenate([-s, s], axis=0).T
            return 0

        lax.fori_loop(0, n // 128, spread, 0)
    m = p = 0
    target = {}
    for t, e in enumerate(turns):
        group = [k for k, task in enumerate(tasks) if task.turn == e]
        for k in group:
            if tasks[k].rows:
                target[k] = turned.at[m]
                m += 1
            else:
                target[k] = outs[tasks[k].to].at[tasks[k].index]
            if k in loads:
                loads.pop(k).wait()

        def rotate(q, _, t=t, group=group):
            r = pl.ds(pl.multiple_of(q * ROWS, ROWS), ROWS)
            c, s = wide_c[t, r, :], wide_s[t, r, :]
            x = [ready[k][r, :].astype(jnp.float32) for k in group]
            w = [pltpu.roll(v, size // 2, 1) for v in x]
            for k, v, u in zip(group, x, w):
                target[k][r, :] = (v * c + u * s).astype(BF16)
            return 0

        lax.fori_loop(0, n // ROWS, rotate, 0, unroll=UNROLL)
    for k, task in enumerate(tasks):
        if k in loads:
            loads[k].wait()
        block = ready[k]
        if task.turn is not None:
            block = target[k]
        elif not task.rows and k not in loads:
            to = outs[task.to].at[task.index]

            def copy(q, _, block=block, to=to):
                r = pl.ds(pl.multiple_of(q * 256, 256), 256)
                to[r, :] = block[r, :]
                return 0

            lax.fori_loop(0, n // 256, copy, 0)
        if not task.rows:
            continue
        ready[k] = block
        index = value_at(task.index, y, z)
        to = outs[task.to].at[pl.ds(pl.multiple_of(index * n, n), n)]
        stores.append(pltpu.make_async_copy(block, to, out_sem.at[k]))
        stores[-1].start()
    count, group = n // PAGE, 16
    for k, task in enumerate(tasks):
        if not task.pages:
            continue

        def bound(q, _, block=ready[k], p=p):
            rows = block[pl.ds(pl.multiple_of(q * group * PAGE, group * PAGE), group * PAGE), :]
            rows = rows.reshape(group, PAGE, size)
            r = pl.ds(pl.multiple_of(q * group, group), group)
            high[p, r, :] = jnp.max(rows, axis=1)
            low[p, r, :] = jnp.min(rows, axis=1)
            return 0

        lax.fori_loop(0, count // group, bound, 0, unroll=True)
        for i, side in enumerate((high, low)):
            to = outs[writes - 2 + i].at[pl.ds(pl.multiple_of(value_at(task.index, y, z) * count, 16), count)]
            stores.append(pltpu.make_async_copy(side.at[p], to, page_sem.at[i, p]))
            stores[-1].start()
        p += 1
    for store in stores:
        store.wait()


def step(far, near, angles, sent, grown, tasks):
    n, size = (*far, *near)[0].shape[-2:]
    turns = sorted({t.turn for t in tasks if t.turn is not None})
    hbm, vmem = pl.BlockSpec(memory_space=pl.ANY), pl.BlockSpec(memory_space=pltpu.VMEM)
    operands = [pltpu.with_memory_space_constraint(a, pltpu.HBM) for a in far]
    operands += [pltpu.with_memory_space_constraint(a, pltpu.VMEM) for a in near]
    in_specs = [hbm] * len(far) + [vmem] * len(near)
    if turns:
        operands.append(pltpu.with_memory_space_constraint(angles, pltpu.HBM))
        in_specs.append(hbm)
    out = [pltpu.VMEM((c, n, size), BF16) for c in sent]
    out_specs = [vmem] * len(sent) + [hbm] * len(grown)
    aliases = {}
    for a in grown:
        if hasattr(a, "dtype"):
            aliases[len(operands)] = len(out)
            operands.append(a)
            in_specs.append(hbm)
            a = a.shape
        out.append(jax.ShapeDtypeStruct(a, BF16))
    t = max(len(turns), 1)
    held = max(sum(k.read < len(far) and (k.turn is not None or k.rows) for k in tasks), 1)
    loads = max(sum(k.read < len(far) for k in tasks), 1)
    m = max(sum(k.turn is not None and k.rows for k in tasks), 1)
    p = max(sum(k.pages for k in tasks), 1)
    f32 = jnp.float32
    return pl.pallas_call(
        functools.partial(step_kernel, len(far), len(near), len(out), len(aliases), tasks, turns),
        out_shape=out,
        in_specs=in_specs,
        out_specs=out_specs,
        input_output_aliases=aliases,
        scratch_shapes=[
            pltpu.VMEM((held, n, size), BF16),
            pltpu.VMEM((m, n, size), BF16),
            pltpu.VMEM((p, n // PAGE, size), BF16),
            pltpu.VMEM((p, n // PAGE, size), BF16),
            pltpu.VMEM((t, size // 2, n), f32),
            pltpu.VMEM((t, n, size), f32),
            pltpu.VMEM((t, n, size), f32),
            pltpu.SemaphoreType.DMA((loads,)),
            pltpu.SemaphoreType.DMA((len(tasks),)),
            pltpu.SemaphoreType.DMA((2, p)),
            pltpu.SemaphoreType.DMA((t,)),
        ],
        cost_estimate=pl.CostEstimate(
            flops=COST * len(tasks), bytes_accessed=4 * len(tasks) * n * size, transcendentals=0
        ),
        compiler_params=pltpu.CompilerParams(vmem_limit_bytes=VMEM_LIMIT),
    )(*operands)


def on_device(fresh_keys, fresh_values, turn_angle):
    keys, values, angles = fresh_keys[:, :, 0], fresh_values[:, :, 0], turn_angle.T
    seqs, n, size = keys.shape
    grown = [(seqs * n, size)] * 2 + [(seqs * n // PAGE, size)] * 2
    near = (1, 3)

    def key_block(e, j):
        return lambda y, z: slot(y + e, z + j)

    def value_block(e, j):
        return lambda y, z: slot(y + j, z + e)

    def from_y(e, j):
        return lambda y, z: slot(y - e, z - j)

    def hop(sent, first, js):
        half = len(sent) // 2
        moved = [shift(a, e if first else 0, 0 if first else e) for a, e in zip(sent[:half], js)]
        return moved, [shift(a, 0 if first else e, e if first else 0) for a, e in zip(sent[half:], js)]

    def pick(es, js):
        tasks = []
        for i, e in enumerate(es):
            tasks += [Task(0, key_block(e, j), i, q) for q, j in enumerate(js)]
        for i, e in enumerate(es):
            tasks += [Task(1, value_block(e, j), len(es) + i, q) for q, j in enumerate(js)]
        sent = step((keys, values), (), None, [len(js)] * (2 * len(es)), [], tasks)
        return hop(sent, True, es)

    k_first, v_first = pick((2,), (0, 1))
    k_rest, v_rest = pick(near, (0, 1, 3, 2))
    second = (1, 3, 2)

    tasks = [Task(0, key_block(0, j), q, 0, 0) for q, j in enumerate(second)]
    tasks += [Task(1, value_block(0, j), 3 + q, 0) for q, j in enumerate(second)]
    tasks.append(Task(0, key_block(0, 0), 6, from_y(0, 0), 0, True, True))
    tasks.append(Task(1, value_block(0, 0), 7, from_y(0, 0), rows=True))
    *sent, a, b, c, d = step((keys, values), (), angles, [1] * 6, grown, tasks)
    grown = [a, b, c, d]
    k_own, v_own = hop(sent[:2] + sent[3:5], False, near)
    k_own2, v_own2 = hop(sent[2:3] + sent[5:6], False, (2,))
    k_far, v_far = pick((2,), (3, 2))

    near_in = (*k_rest, *v_rest)
    tasks = []
    for q in range(3):
        tasks += [Task(i, 1 + q, q, i, e) for i, e in enumerate(near)]
        tasks += [Task(2 + i, 1 + q, 3 + q, i) for i, e in enumerate(near)]
    tasks += [Task(i, 0, 6, from_y(e, 0), e, True, True) for i, e in enumerate(near)]
    tasks += [Task(2 + i, 0, 7, from_y(0, e), rows=True) for i, e in enumerate(near)]
    *sent, a, b, c, d = step((), near_in, angles, [2] * 6, grown, tasks)
    grown = [a, b, c, d]
    k_near, v_near = hop(sent[:2] + sent[3:5], False, near)
    k_near2, v_near2 = hop(sent[2:3] + sent[5:6], False, (2,))

    parts = ((0, 1), (2, 0), (2, 1))
    tasks = [Task(i, at, q, 0, 2) for q, (i, at) in enumerate(parts)]
    tasks += [Task(i + 1, at, 3 + q, 0) for q, (i, at) in enumerate(parts)]
    tasks.append(Task(0, 0, 6, from_y(2, 0), 2, True, True))
    tasks.append(Task(1, 0, 7, from_y(0, 2), rows=True))
    far_in = (*k_first, *v_first, *k_far, *v_far)
    *sent, a, b, c, d = step((), far_in, angles, [1] * 6, grown, tasks)
    grown = [a, b, c, d]
    k_last, v_last = hop(sent[:2] + sent[3:5], False, near)
    k_last2, v_last2 = hop(sent[2:3] + sent[5:6], False, (2,))

    def finish(got, grown):
        tasks, reads = [], []
        for k_got, v_got, js, es in got:
            for a, b, j in zip(k_got, v_got, js):
                at = len(reads)
                reads += [a, b]
                tasks += [Task(at, q, 0, from_y(e, j), None, True, True) for q, e in enumerate(es)]
                tasks += [Task(at + 1, q, 1, from_y(j, e), None, True) for q, e in enumerate(es)]
        return step((), reads, None, [], grown, tasks)

    grown = finish([(k_own, v_own, near, (0,)), (k_own2, v_own2, (2,), (0,))], grown)
    grown = finish([(k_near, v_near, near, near), (k_near2, v_near2, (2,), near)], grown)
    grown = finish([(k_last, v_last, near, (2,))], grown)
    grown = finish([(k_last2, v_last2, (2,), (2,))], grown)
    return tuple(x[None, :, None] for x in grown)


def solution(mesh):
    cut = P(None, SEQ, "model", None)
    out = P(SEQ, None, "model", None)

    return jax.shard_map(on_device, mesh=mesh, in_specs=(cut, cut, P()), out_specs=(out,) * 4, check_vma=False)
```
